32 devices in a mesh: grp: 2 (over x), shard: 16 (over z, y, core).
Axes of the slice: x: 2, y: 2, z: 4, core: 2. Of those that a mesh axis runs over, the one named last changes fastest.
Arguments:
- window: bfloat16 [32, 4096], P('grp'), may hold values from -6 to 6
- weight: bfloat16 [11008, 4096], P('shard'), may hold values from -0.09375 to 0.09375
- factor_a: bfloat16 [64, 4, 4096], P(('grp', 'shard')), may hold values from -6 to 6
- factor_b: bfloat16 [64, 4, 11008], P(('grp', 'shard')), may hold values from -6 to 6
- fitness: float32 [64], P(('grp', 'shard')), may hold values from -4 to 4
Outputs:
- perturbed: bfloat16 [11008, 1024], P('shard', 'grp')
- update: float32 [11008, 4096], P('shard', 'grp')
The draws below stay inside these ranges and needn't reach their ends.
All inputs are finite; a program needn't handle non-finite values.
Results may differ from the reference program's by a relative error of at most 0.0029.
Values may be sent and summed in bfloat16 or wider, within the bound.
A program may use at most 64 MiB of HBM per device.

```python
import math
import jax
import jax.numpy as jnp
from jax import lax

D = 4096
FF = 11008
TOK = 16
RANK = 4
CANDS = 64
N_GRP = 2


def levels(rng, extent, split, smallest, high):
    def one(dim, blocks):
        draws = jax.random.uniform(jax.random.fold_in(jax.random.fold_in(rng, 6), dim), (blocks,), jnp.float32, smallest / len(split), high / len(split))
        return jnp.repeat(jnp.exp(draws), extent[dim] // blocks).reshape((-1,) + (1,) * (len(extent) - dim - 1))

    level = one(*split[0])
    for cut in split[1:]:
        level = level * one(*cut)
    return level


def normal_values(own_key, shape, width, most, pieces=(), kind=jnp.bfloat16):
    gain = levels(own_key, shape, pieces, -0.22, 0.18) if pieces else 1.0
    values = jax.random.normal(own_key, shape, jnp.float32) * width * gain
    return jnp.minimum(jnp.maximum(values, -most), most).astype(kind)


def setup_inputs(seed: int = 0) -> dict:
    streams_of = jax.random.split(jax.random.key(seed), 6)
    window = normal_values(streams_of[0], (N_GRP * TOK, D), 1.0, 6.0, ((0, 2),))
    weight = normal_values(streams_of[1], (FF, D), D ** -0.5, 0.09375, ((0, 16),))
    factor_a = normal_values(streams_of[2], (CANDS, RANK, D), 1.0, 6.0, ((0, 32),))
    factor_b = normal_values(streams_of[3], (CANDS, RANK, FF), 1.0, 6.0, ((0, 32),))
    fitness = normal_values(streams_of[4], (CANDS,), 1.0, 4.0, ((0, 32),), jnp.float32)
    return {"window": window, "weight": weight, "factor_a": factor_a, "factor_b": factor_b, "fitness": fitness}


def reference(window, weight, factor_a, factor_b, fitness):
    total_cands = factor_a.shape[0]
    group_count = window.shape[0] // TOK
    per_group = total_cands // group_count
    perturb = 0.25 / math.sqrt(D)
    base_out = jnp.dot(window, weight.T, preferred_element_type=jnp.float32).reshape(group_count, TOK, FF)
    x_groups = window.reshape(group_count, TOK, D)
    a_groups = factor_a.reshape(group_count, per_group, RANK, D)
    b_groups = factor_b.reshape(group_count, per_group, RANK, FF)

    def one_group(inputs):
        group_window, group_a, group_b, group_base = inputs
        projected = jnp.einsum('td,crd->crt', group_window.astype(jnp.float32), group_a.astype(jnp.float32), precision=lax.Precision.HIGHEST)
        low_rank = jnp.einsum('crt,crf->ctf', projected, group_b.astype(jnp.float32), precision=lax.Precision.HIGHEST)
        return (group_base[None] + perturb * low_rank).astype(jnp.bfloat16)
    perturbed = lax.map(one_group, (x_groups, a_groups, b_groups, base_out)).reshape(total_cands * TOK, FF).T
    weighted = (fitness[:, None, None] * factor_b.astype(jnp.float32)).astype(jnp.bfloat16)
    update = jnp.dot(weighted.reshape(total_cands * RANK, FF).T, factor_a.reshape(total_cands * RANK, D), preferred_element_type=jnp.float32)
    update = update * (0.5 / math.sqrt(total_cands))
    return (perturbed, update)
```

```python
import functools
import math

import jax
import jax.numpy as jnp
from jax import lax
from jax.experimental import pallas as pl
from jax.experimental.pallas import tpu as pltpu
from jax.sharding import PartitionSpec as P

MESH = pl.DeviceIdType.MESH
F32 = jnp.float32
BF16 = jnp.bfloat16
ROW_CHUNK = 256
COL_BLOCK = 512


def dot_rows(left, right):
    return lax.dot_general(left, right, (((1,), (1,)), ((), ())), preferred_element_type=F32)


def dot_cols(left, right):
    return lax.dot_general(left, right, (((0,), (0,)), ((), ())), preferred_element_type=F32)


def split3(v):
    high = v.astype(BF16)
    rest = v - high.astype(F32)
    mid = rest.astype(BF16)
    low = (rest - mid.astype(F32)).astype(BF16)
    return high, mid, low


def exchange_kernel(
    n_grp, n_shard, perturb, fit_hbm, win_hbm, a_hbm, b_hbm, weight_ref,
    a_all, weighted, pert_ref,
    fit_ref, win_ref, a_ref, b_ref, in_sem,
    a_rows, b_slabs, b_all, weight, w_sem, b_send, b_recv, b_send_x, b_recv_x,
    a_send, a_send_z, a_send_y, a_send_c, a_recv, a_recv_z, a_recv_y, a_recv_c,
):
    depth = n_shard // 8
    count = n_grp * n_shard
    line = n_grp * depth
    grp = lax.axis_index("grp")
    shard = lax.axis_index("shard")
    core = shard % 2
    y = (shard // 2) % 2
    low_z = (shard // 4) % 2
    high_z = shard // 8
    half = a_all.shape[2]
    cand_dev, rank, _ = a_ref.shape
    rows = cand_dev * rank
    ff = weight_ref.shape[0]
    tok = win_ref.shape[0]
    wide = b_all.shape[2]
    cols = pert_ref.shape[1]

    def slot_of(c, yy, lz, i):
        return i // depth * n_shard + ((c * 2 + yy) * 2 + lz) * depth + i % depth

    def slot_at(s):
        return slot_of(s % 2, s // 2 % 2, s // 4 % 2, grp * depth + s // 8)

    own = slot_at(shard)

    inputs = [
        pltpu.make_async_copy(src, dst, in_sem.at[i])
        for i, (src, dst) in enumerate(
            [(a_hbm, a_ref), (b_hbm, b_ref), (win_hbm, win_ref), (fit_hbm, fit_ref)]
        )
    ]
    for load in inputs:
        load.start()

    barrier = pltpu.get_barrier_semaphore()

    def line_peer(i):
        return ((grp + i // depth) % n_grp, (high_z + i) % depth * 8 + low_z * 4 + y * 2 + core)

    def greet_shard(i, carry):
        pl.semaphore_signal(
            barrier, inc=1, device_id=(grp, (shard + i) % n_shard), device_id_type=MESH
        )
        return carry

    def greet_line(i, carry):
        pl.semaphore_signal(barrier, inc=1, device_id=line_peer(i), device_id_type=MESH)
        return carry

    lax.fori_loop(1, n_shard, greet_shard, 0)
    lax.fori_loop(depth, line, greet_line, 0)

    chunks = [(lo, min(ROW_CHUNK, ff - lo)) for lo in range(0, ff, ROW_CHUNK)]
    loads = [
        pltpu.make_async_copy(
            weight_ref.at[pl.ds(lo, size)], weight.at[pl.ds(lo, size)], w_sem.at[i]
        )
        for i, (lo, size) in enumerate(chunks)
    ]
    for load in loads:
        load.start()

    inputs[0].wait()
    a_rows[...] = jnp.concatenate(
        [a_ref[j].astype(F32) for j in range(cand_dev)], axis=0
    ).astype(BF16)

    pl.semaphore_wait(barrier, n_shard - 1 + line - depth)

    def origin(i):
        g = (grp + n_grp - i // depth) % n_grp
        return g * depth + (high_z + depth - i % depth) % depth

    def a_source(g):
        return a_rows.at[:, pl.ds(pl.multiple_of(g * half, half), half)]

    def send_a(i, carry):
        pltpu.make_async_remote_copy(
            src_ref=a_source((grp + i // depth) % n_grp),
            dst_ref=a_all.at[own],
            send_sem=a_send,
            recv_sem=a_recv.at[i],
            device_id=line_peer(i),
            device_id_type=MESH,
        ).start()
        return carry

    def send_b(i, carry):
        to = (shard + i) % n_shard
        pltpu.make_async_remote_copy(
            src_ref=b_slabs.at[to],
            dst_ref=b_all.at[own],
            send_sem=b_send,
            recv_sem=b_recv.at[i],
            device_id=(grp, to),
            device_id_type=MESH,
        ).start()
        return carry

    def cross_b(src, slot):
        def one(k, carry):
            pltpu.make_async_remote_copy(
                src_ref=src,
                dst_ref=b_all.at[slot],
                send_sem=b_send_x,
                recv_sem=b_recv_x,
                device_id=((grp + k) % n_grp, shard),
                device_id_type=MESH,
            ).start()
            return carry

        lax.fori_loop(1, n_grp, one, 0)

    def wait_bytes(ref, sem):
        pltpu.make_async_copy(ref, ref, sem).wait()

    def relay_b(i, carry):
        wait_bytes(b_all.at[0], b_recv.at[i])
        slot = slot_at((shard + n_shard - i) % n_shard)
        cross_b(b_all.at[slot], slot)
        return carry

    def forward(src, slot, c, yy, lz, send_sem, recv_sem):
        pltpu.make_async_remote_copy(
            src_ref=src,
            dst_ref=a_all.at[slot],
            send_sem=send_sem,
            recv_sem=recv_sem,
            device_id=(grp, high_z * 8 + lz * 4 + yy * 2 + c),
            device_id_type=MESH,
        ).start()

    def spread_a(src, slot, i):
        forward(src, slot, core, y, 1 - low_z, a_send_z, a_recv_z.at[i])
        forward(src, slot, core, 1 - y, low_z, a_send_y, a_recv_y.at[i])
        forward(src, slot, 1 - core, y, low_z, a_send_c, a_recv_c)

    def relay(i, carry):
        wait_bytes(a_all.at[0], a_recv.at[i])
        slot = slot_of(core, y, low_z, origin(i))
        spread_a(a_all.at[slot], slot, i)
        return carry

    def relay_z(i, carry):
        wait_bytes(a_all.at[0], a_recv_z.at[i])
        slot = slot_of(core, y, 1 - low_z, origin(i))
        forward(a_all.at[slot], slot, core, 1 - y, low_z, a_send_y, a_recv_y.at[line + i])
        forward(a_all.at[slot], slot, 1 - core, y, low_z, a_send_c, a_recv_c)
        return carry

    def relay_y(i, carry):
        wait_bytes(a_all.at[0], a_recv_y.at[i])
        lz = (low_z + i // line) % 2
        slot = slot_of(core, 1 - y, lz, origin(i % line))
        forward(a_all.at[slot], slot, 1 - core, y, low_z, a_send_c, a_recv_c)
        return carry

    lax.fori_loop(1, line, send_a, 0)
    spread_a(a_source(grp), own, 0)

    for load in inputs[1:]:
        load.wait()
    projected = dot_rows(a_rows[...], win_ref[...]) * perturb
    high = projected.astype(BF16)
    low = (projected - high.astype(F32)).astype(BF16)
    row = lax.broadcasted_iota(jnp.int32, (rows, 1), 0)
    fit = jnp.zeros((rows, 1), F32)
    for j in range(cand_dev):
        fit = jnp.where(row // rank == j, fit_ref[j], fit)
    extra = [high, low, *split3(fit)]
    extra.append(jnp.zeros((rows, wide - ff - sum(v.shape[1] for v in extra)), BF16))
    extra = jnp.concatenate([v.astype(F32) for v in extra], axis=1)
    for k in range(n_shard):
        slab = jnp.concatenate(
            [b_ref[j, :, k * ff : (k + 1) * ff].astype(F32) for j in range(cand_dev)], axis=0
        )
        b_slabs[k] = jnp.concatenate([slab, extra], axis=1).astype(BF16)

    lax.fori_loop(1, n_shard, send_b, 0)
    cross_b(b_slabs.at[shard], own)
    b_all[own] = b_slabs[shard]
    a_all[own] = a_rows[:, pl.ds(pl.multiple_of(grp * half, half), half)]

    parts = []
    for (lo, size), load in zip(chunks, loads):
        load.wait()
        parts.append(dot_rows(win_ref[...], weight[pl.ds(lo, size)]))
    base = jnp.concatenate(split3(jnp.concatenate(parts, axis=1)), axis=0)

    def relay_far(j, carry):
        return relay(j // (depth - 1) * depth + j % (depth - 1) + 1, carry)

    lax.fori_loop(0, 1, relay_z, 0)
    lax.fori_loop(0, 1, relay_y, 0)
    lax.fori_loop(1, n_grp, lambda k, carry: relay(k * depth, carry), 0)
    if depth > 1:
        lax.fori_loop(0, n_grp * (depth - 1), relay_far, 0)
    lax.fori_loop(1, n_shard // 2, relay_b, 0)
    lax.fori_loop(1, line, relay_z, 0)
    lax.fori_loop(n_shard // 2, n_shard, relay_b, 0)
    lax.fori_loop(1, 2 * line, relay_y, 0)

    wait_bytes(b_all.at[pl.ds(0, count - n_shard)], b_recv_x)

    lane = lax.broadcasted_iota(jnp.int32, (count, rows, wide - ff), 2)
    every = b_all[:, :, ff:].astype(F32)
    scale = jnp.sum(
        jnp.where((lane >= 2 * tok) & (lane < 2 * tok + 3), every, 0.0), axis=2, keepdims=True
    )
    scaled = b_all[:, :, :ff].astype(F32) * scale
    weighted[...] = scaled.reshape(count * rows, ff).astype(BF16)

    mine = pl.ds(grp * n_shard, n_shard)
    k = n_shard * rows
    own_b = b_all[mine, :, :ff].astype(F32).reshape(k, ff).astype(BF16)
    start = ff // 128 * 128
    codes = b_all[mine, :, start:].astype(F32).reshape(k, wide - start).astype(BF16)
    r = lax.broadcasted_iota(jnp.int32, (k, cols), 0)
    slab = r // rows
    cyz = slab // depth
    sh = (slab % depth) * 8 + (cyz % 2) * 4 + (cyz // 2 % 2) * 2 + cyz // 4
    cand = sh * cand_dev + (r % rows) // rank
    same = cand == lax.broadcasted_iota(jnp.int32, (k, cols), 1) // tok

    def pick(depth_in, first):
        at = lax.broadcasted_iota(jnp.int32, (depth_in, cols), 0) - first
        to = lax.broadcasted_iota(jnp.int32, (depth_in, cols), 1) % tok
        return at, to

    def blocks(first):
        at, to = pick(wide - start, ff - start + first)
        chosen = (at == to).astype(F32).astype(BF16)
        spread = jnp.dot(codes, chosen, preferred_element_type=F32)
        return jnp.where(same, spread, 0.0).astype(BF16)

    at, to = pick(3 * tok, 0)
    total = dot_cols(base, (at % tok == to).astype(F32).astype(BF16))
    total = total + dot_cols(own_b, blocks(0)) + dot_cols(own_b, blocks(tok))
    pert_ref[...] = total.astype(BF16)

    wait_bytes(a_all.at[pl.ds(0, 4 * line)], a_recv_c)
    wait_bytes(b_all.at[pl.ds(0, count - n_shard)], b_send_x)
    wait_bytes(a_all.at[pl.ds(0, line - 1)], a_send)
    wait_bytes(a_all.at[pl.ds(0, line)], a_send_z)
    wait_bytes(a_all.at[pl.ds(0, 2 * line)], a_send_y)
    wait_bytes(a_all.at[pl.ds(0, 4 * line)], a_send_c)
    wait_bytes(b_all.at[pl.ds(0, n_shard - 1)], b_send)


def combine_kernel(step_scale, a_ref, weighted, pert_ref, pert_out, upd_out, upd, p_sem, u_sem):
    count, rows, half = a_ref.shape
    store = pltpu.make_async_copy(pert_ref, pert_out, p_sem)
    store.start()
    stores = []
    for n, lo in enumerate(range(0, half, COL_BLOCK)):
        at = pl.ds(lo, min(COL_BLOCK, half - lo))
        block = a_ref[:, :, at].reshape(count * rows, at.size)
        upd[:, at] = dot_cols(weighted[...], block) * step_scale
        stores.append(pltpu.make_async_copy(upd.at[:, at], upd_out.at[:, at], u_sem.at[n]))
        stores[-1].start()
    store.wait()
    for done in stores:
        done.wait()


def local(window, weight, factor_a, factor_b, fitness):
    tok, model_width = window.shape
    cand_dev, rank, _ = factor_a.shape
    n_shard = lax.axis_size("shard")
    n_grp = lax.axis_size("grp")
    total_cands = cand_dev * n_grp * n_shard
    perturb = 0.25 / math.sqrt(model_width)
    step_scale = 0.5 / math.sqrt(total_cands)
    rows = cand_dev * rank
    ff = weight.shape[0]
    half = model_width // n_grp
    count = n_grp * n_shard
    line = n_grp * (n_shard // 8)
    wide = -(-(ff + 2 * tok + 3) // 128) * 128
    cols = n_shard * cand_dev * tok

    operands = (fitness, window, factor_a, factor_b, weight)
    n_chunks = -(-ff // ROW_CHUNK)
    vmem = pl.BlockSpec(memory_space=pltpu.VMEM)
    hbm = pl.BlockSpec(memory_space=pltpu.HBM)
    dma = pltpu.SemaphoreType.DMA
    a_all, weighted, pert = pl.pallas_call(
        functools.partial(exchange_kernel, n_grp, n_shard, perturb),
        out_shape=(
            jax.ShapeDtypeStruct((count, rows, half), BF16),
            jax.ShapeDtypeStruct((count * rows, ff), BF16),
            jax.ShapeDtypeStruct((ff, cols), BF16),
        ),
        in_specs=[hbm] * 5,
        out_specs=(vmem, vmem, vmem),
        scratch_shapes=[
            pltpu.SMEM(fitness.shape, F32),
            pltpu.VMEM(window.shape, BF16),
            pltpu.VMEM(factor_a.shape, BF16),
            pltpu.VMEM(factor_b.shape, BF16),
            dma((4,)),
            pltpu.VMEM((rows, model_width), BF16),
            pltpu.VMEM((n_shard, rows, wide), BF16),
            pltpu.VMEM((count, rows, wide), BF16),
            pltpu.VMEM((ff, model_width), BF16),
            dma((n_chunks,)),
            dma, dma((n_shard,)), dma, dma, dma, dma, dma, dma,
            dma((line,)), dma((line,)), dma((2 * line,)), dma,
        ],
        compiler_params=pltpu.CompilerParams(
            collective_id=0, has_side_effects=True, vmem_limit_bytes=50 * 1024 * 1024
        ),
        name="exchange",
    )(*[pltpu.with_memory_space_constraint(v, pltpu.HBM) for v in operands])

    perturbed, update = pl.pallas_call(
        functools.partial(combine_kernel, step_scale),
        out_shape=(
            jax.ShapeDtypeStruct((ff, cols), BF16),
            jax.ShapeDtypeStruct((ff, half), F32),
        ),
        in_specs=[vmem, vmem, vmem],
        out_specs=(hbm, hbm),
        scratch_shapes=[pltpu.VMEM((ff, half), F32), dma, dma((-(-half // COL_BLOCK),))],
        compiler_params=pltpu.CompilerParams(vmem_limit_bytes=40 * 1024 * 1024),
        name="combine",
    )(a_all, weighted, pert)
    return perturbed, update


def solution(mesh):
    in_specs = (
        P("grp", None),
        P("shard", None),
        P(("grp", "shard"), None, None),
        P(("grp", "shard"), None, None),
        P(("grp", "shard")),
    )
    out_specs = (P("shard", "grp"), P("shard", "grp"))
    return jax.shard_map(local, mesh=mesh, in_specs=in_specs, out_specs=out_specs, check_vma=False)
```
